32 devices in a mesh: grp: 4 (over y, x), dev: 8 (over z, core).
Axes of the slice: x: 2, y: 2, z: 4, core: 2. Of those that a mesh axis runs over, the one named last changes fastest.
Arguments:
- examples: float32 [2048, 32768], P(('grp', 'dev'))
- labels: int32 [2048], P(('grp', 'dev')), may hold values from 0 to 1, as said below
Outputs:
- consensus: float32 [32768], replicated
- local_weights: float32 [32, 32768], P(('grp', 'dev'))
- dual_vars: float32 [32, 32768], P(('grp', 'dev'))
The draws below stay inside these ranges and needn't reach their ends.
Inputs may be any that keep to these rules, and one draw needn't show every extreme that they name: `labels`: each example's class, 0 or 1.
All inputs are finite; a program needn't handle non-finite values.
Results may differ from the reference program's by a relative error of at most 0.00012.
Values sent between devices are 32-bit elements; how exact they have to be, the bound alone decides.
A program may use at most 64 MiB of HBM per device.

```python
import jax
import jax.numpy as jnp
from jax import lax

F = 32768
ROWS = 64
PROX = 3
ROUNDS = 4
TOTAL_ROWS = 2048
N_GRP = 4
N_DEV = 8


def label_keys(key):
    base = jax.random.fold_in(key, 7)
    label_key, noise_key, direction_random_key = jax.random.split(base, 3)
    classes = jax.random.randint(label_key, (TOTAL_ROWS,), 0, 2).astype(jnp.int32)
    return (classes, noise_key, direction_random_key)


def draw_labels(key, part):
    classes, noise_key, direction_random_key = label_keys(key)
    return classes


def draw_examples(key, part):
    classes, noise_key, direction_random_key = label_keys(key)
    direction = jax.random.normal(direction_random_key, (F,), jnp.float32)
    polarity = 2.0 * classes.astype(jnp.float32) - 1.0
    strength = 0.6 / jnp.sqrt(jnp.float32(ROWS))
    noise_part = jax.random.normal(noise_key, (TOTAL_ROWS, F), jnp.float32)
    values = noise_part + strength * polarity[:, None] * direction[None, :]
    values = values / (10.0 * jnp.sqrt(jnp.float32(F)))
    return values.astype(jnp.float32)


def setup_inputs(seed: int = 0) -> dict:
    key_list = jax.random.split(jax.random.key(seed), 3)
    return {
        "examples": draw_examples(jax.random.fold_in(key_list[2], 71), 0),
        "labels": draw_labels(jax.random.fold_in(key_list[2], 71), 0),
    }


step_size = 200.0
penalty = 0.005
thresh = 0.04


def shrink(values):
    return values - jnp.clip(values, -thresh, thresh)


def reference(examples, labels):
    members = N_GRP * N_DEV
    example_blocks = examples.reshape(members, ROWS, F)
    targets = labels.reshape(members, ROWS).astype(jnp.float32)

    def one_round(round_index, carried):
        consensus, weight_vector, dual_vars = carried
        consensus_point = consensus[None, :] - dual_vars
        for prox_index in range(PROX):
            label_margins = jnp.einsum("guz,gz->gu", example_blocks, weight_vector, precision=lax.Precision.HIGHEST)
            primal_residual = jax.nn.sigmoid(label_margins) - targets
            loss_gradient = jnp.einsum("pjl,pj->pl", example_blocks, primal_residual, precision=lax.Precision.HIGHEST)
            weight_vector = (weight_vector - step_size * loss_gradient + step_size * penalty * consensus_point) / (1.0 + step_size * penalty)
        average = jnp.sum(weight_vector + dual_vars, axis=0) / members
        consensus = shrink(average)
        dual_vars = dual_vars + weight_vector - consensus[None, :]
        return consensus, weight_vector, dual_vars

    start = (jnp.zeros((F,), jnp.float32), jnp.zeros((members, F), jnp.float32), jnp.zeros((members, F), jnp.float32))
    consensus, weight_vector, dual_vars = lax.fori_loop(0, ROUNDS, one_round, start)
    return consensus, weight_vector, dual_vars
```

```python
import functools

import jax
import jax.numpy as jnp
from jax import lax
from jax.experimental import pallas as pl
from jax.experimental.pallas import tpu as pltpu
from jax.sharding import PartitionSpec as P

PROX = 3
ROUNDS = 4
step_size = 200.0
penalty = 0.005
thresh = 0.04
shrinkage = 1.0 + step_size * penalty

LANES = 128
SUB = 8
GROUP = LANES * SUB
MESH = pl.DeviceIdType.MESH


def kernel(
    n_grp, n_dev, cores,
    x_hbm, labels_ref,
    z_out, w_out, u_out,
    x, w, u, v, comb, arrived, partial, zfull, gram,
    load_sem, rs_send, rs_recv, line_send, line_recv, ag_send, ag_recv, out_sem,
):
    rows = x.shape[1]
    blocks = x.shape[0]
    plane = n_grp * cores
    line = n_dev // cores
    per = blocks // plane
    members = n_grp * n_dev

    grp = lax.axis_index("grp")
    dev = lax.axis_index("dev")
    core = lax.rem(dev, cores)
    depth = lax.div(dev, cores)
    own = grp * cores + core

    def plane_peer(offset):
        a, b = offset // cores, offset % cores
        other_grp = lax.rem(grp + a, n_grp)
        other_core = lax.rem(core + b, cores)
        return (other_grp, depth * cores + other_core), other_grp * cores + other_core

    def line_peer(offset):
        return (grp, lax.rem(depth + offset, line) * cores + core)

    def load(i):
        return pltpu.make_async_copy(
            x_hbm.at[:, pl.ds(pl.multiple_of(i * GROUP, GROUP), GROUP)], x.at[i], load_sem.at[i]
        )

    def start_load(i, carry):
        load(i).start()
        return carry

    lax.fori_loop(0, blocks, start_load, 0)

    barrier = pltpu.get_barrier_semaphore()
    for offset in range(1, plane):
        pl.semaphore_signal(barrier, inc=1, device_id=plane_peer(offset)[0], device_id_type=MESH)
    for offset in range(1, line):
        pl.semaphore_signal(barrier, inc=1, device_id=line_peer(offset), device_id_type=MESH)

    eye = (
        lax.broadcasted_iota(jnp.int32, (rows, rows), 0) == lax.broadcasted_iota(jnp.int32, (rows, rows), 1)
    ).astype(jnp.float32)
    targets = jnp.sum(eye * labels_ref[...].astype(jnp.float32), axis=1, keepdims=True)

    gram[...] = jnp.zeros_like(gram)
    for ref in (w, u, v):
        ref[...] = jnp.zeros_like(ref)

    def gram_block(i, carry):
        load(i).wait()
        value = x[i]
        high = value.astype(jnp.bfloat16)
        low = (value - high.astype(jnp.float32)).astype(jnp.bfloat16)
        both = jnp.concatenate([high, low], axis=0)
        gram[...] += lax.dot_general(
            both, both, (((1,), (1,)), ((), ())), preferred_element_type=jnp.float32
        )
        return carry

    lax.fori_loop(0, blocks, gram_block, 0)
    full = gram[...]
    g = (full[:rows, :rows] + full[rows:, rows:]) + (full[:rows, rows:] + full[rows:, :rows])

    pl.semaphore_wait(barrier, plane - 1 + line - 1)

    def rs_copy(t, offset):
        device, chunk = plane_peer(offset)
        return pltpu.make_async_remote_copy(
            src_ref=comb.at[pl.ds(chunk * per, per)],
            dst_ref=arrived.at[t, offset - 1],
            send_sem=rs_send.at[t, offset - 1],
            recv_sem=rs_recv.at[t, offset - 1],
            device_id=device,
            device_id_type=MESH,
        )

    def line_copy(t, offset):
        return pltpu.make_async_remote_copy(
            src_ref=partial.at[t, depth],
            dst_ref=partial.at[t, depth],
            send_sem=line_send.at[t, offset - 1],
            recv_sem=line_recv.at[t, offset - 1],
            device_id=line_peer(offset),
            device_id_type=MESH,
        )

    def ag_copy(t, offset):
        device, _ = plane_peer(offset)
        return pltpu.make_async_remote_copy(
            src_ref=zfull.at[t, pl.ds(own * per, per)],
            dst_ref=zfull.at[t, pl.ds(own * per, per)],
            send_sem=ag_send.at[t, offset - 1],
            recv_sem=ag_recv.at[t, offset - 1],
            device_id=device,
            device_id_type=MESH,
        )

    def local_steps(xw, xv):
        total = jnp.zeros_like(xw)
        for prox_index in range(PROX):
            residual = jax.nn.sigmoid(xw) - targets
            across = jnp.sum(eye * residual, axis=0, keepdims=True)
            gr = jnp.sum(g * across, axis=1, keepdims=True)
            xw = (xw - step_size * gr + step_size * penalty * xv) / shrinkage
            total = (total + step_size * residual) / shrinkage
        return xw, total

    w_keep = 1.0 / shrinkage**PROX
    v_gain = step_size * penalty * sum(1.0 / shrinkage ** (k + 1) for k in range(PROX))

    def weights_of(chunk, spread):
        def block(j, carry):
            i = chunk * per + j
            sums = []
            for lane in range(SUB):
                cols = slice(lane * LANES, (lane + 1) * LANES)
                acc = x[i, 0:SUB, cols] * spread[0:SUB]
                for k in range(SUB, rows, SUB):
                    acc += x[i, k : k + SUB, cols] * spread[k : k + SUB]
                sums.append(jnp.sum(acc, axis=0, keepdims=True))
            gradient = jnp.concatenate(sums, axis=0)
            fresh = w_keep * w[i] + v_gain * v[i] - gradient
            w[i] = fresh
            comb[i] = fresh + u[i]
            return carry

        lax.fori_loop(0, per, block, 0)

    def margins_of(t, chunk, accs):
        def block(j, accs):
            i = chunk * per + j
            out = list(accs)
            z = zfull[t, i]
            fresh = comb[i] - z
            u[i] = fresh
            v[i] = z - fresh
            for lane in range(SUB):
                cols = slice(lane * LANES, (lane + 1) * LANES)
                row = jnp.broadcast_to(z[lane : lane + 1], (SUB, LANES))
                for k in range(rows // SUB):
                    out[k] = out[k] + x[i, k * SUB : (k + 1) * SUB, cols] * row
            return tuple(out)

        return lax.fori_loop(0, per, block, accs)

    def duals_of(t, chunk):
        def block(j, carry):
            i = chunk * per + j
            u[i] = comb[i] - zfull[t, i]
            return carry

        lax.fori_loop(0, per, block, 0)

    order = list(range(plane - 1, 0, -1))

    def reduce_round(t, total):
        spread = jnp.broadcast_to(total, (rows, LANES))
        for offset in order:
            weights_of(plane_peer(offset)[1], spread)
            rs_copy(t, offset).start()
        weights_of(own, spread)
        mine = comb[pl.ds(own * per, per)]
        for offset in order[::-1]:
            rs_copy(t, offset).wait_recv()
            mine = mine + arrived[t, offset - 1]
        partial[t, depth] = mine
        for offset in range(1, line):
            line_copy(t, offset).start()
        for offset in range(1, line):
            line_copy(t, offset).wait_recv()
        a = partial[t, 0]
        for k in range(1, line):
            a = a + partial[t, k]
        a = a * (1.0 / members) if members & (members - 1) == 0 else a / members
        zfull[t, pl.ds(own * per, per)] = a - jnp.clip(a, -thresh, thresh)
        for offset in order:
            ag_copy(t, offset).start()

    def sends_done(t):
        for offset in range(1, plane):
            rs_copy(t, offset).wait_send()
            ag_copy(t, offset).wait_send()
        for offset in range(1, line):
            line_copy(t, offset).wait_send()

    def source(offset):
        a, b = offset // cores, offset % cores
        return lax.rem(grp + n_grp - a, n_grp) * cores + lax.rem(core + cores - b, cores)

    def one_round(t, carried):
        xw, xu, xz = carried
        xw, total = local_steps(xw, xz - xu)
        reduce_round(t, total)
        accs = tuple(jnp.zeros((SUB, LANES), jnp.float32) for _ in range(rows // SUB))
        accs = margins_of(t, own, accs)
        for offset in order[::-1]:
            ag_copy(t, offset).wait_recv()
            accs = margins_of(t, source(offset), accs)
        fresh_xz = jnp.sum(jnp.concatenate(accs, axis=0), axis=1, keepdims=True)
        sends_done(t)
        return xw, xu + xw - fresh_xz, fresh_xz

    zero = jnp.zeros((rows, 1), jnp.float32)
    xw, xu, xz = lax.fori_loop(0, ROUNDS - 1, one_round, (zero, zero, zero))

    last = ROUNDS - 1
    _, total = local_steps(xw, xz - xu)
    reduce_round(last, total)
    w_copy = pltpu.make_async_copy(w, w_out, out_sem.at[2 * plane])
    w_copy.start()

    def finish(chunk, slot):
        duals_of(last, chunk)
        span = pl.ds(chunk * per, per)
        copies = (
            pltpu.make_async_copy(zfull.at[last, span], z_out.at[span], out_sem.at[2 * slot]),
            pltpu.make_async_copy(u.at[span], u_out.at[span], out_sem.at[2 * slot + 1]),
        )
        for copy in copies:
            copy.start()
        return copies

    pending = [w_copy, *finish(own, 0)]
    for offset in order[::-1]:
        ag_copy(last, offset).wait_recv()
        pending += finish(source(offset), offset)
    sends_done(last)
    for copy in pending:
        copy.wait()


def per_device(n_grp, n_dev, examples, labels):
    rows, width = examples.shape
    cores = 2 if n_dev % 2 == 0 else 1
    plane, line = n_grp * cores, n_dev // cores
    blocks = width // GROUP
    per = blocks // plane
    vector = jax.ShapeDtypeStruct((blocks, SUB, LANES), jnp.float32)
    anywhere = pl.BlockSpec(memory_space=pltpu.HBM)
    vec = pltpu.VMEM((blocks, SUB, LANES), jnp.float32)
    dma = pltpu.SemaphoreType.DMA
    z, w, u = pl.pallas_call(
        functools.partial(kernel, n_grp, n_dev, cores),
        out_shape=(vector, vector, vector),
        in_specs=[anywhere, pl.BlockSpec(memory_space=pltpu.VMEM)],
        out_specs=(anywhere, anywhere, anywhere),
        scratch_shapes=[
            pltpu.VMEM((blocks, rows, GROUP), jnp.float32),
            vec, vec, vec, vec,
            pltpu.VMEM((ROUNDS, plane - 1, per, SUB, LANES), jnp.float32),
            pltpu.VMEM((ROUNDS, line, per, SUB, LANES), jnp.float32),
            pltpu.VMEM((ROUNDS, blocks, SUB, LANES), jnp.float32),
            pltpu.VMEM((2 * rows, 2 * rows), jnp.float32),
            dma((blocks,)),
            dma((ROUNDS, plane - 1)), dma((ROUNDS, plane - 1)),
            dma((ROUNDS, line - 1)), dma((ROUNDS, line - 1)),
            dma((ROUNDS, plane - 1)), dma((ROUNDS, plane - 1)),
            dma((2 * plane + 1,)),
        ],
        compiler_params=pltpu.CompilerParams(collective_id=0, has_side_effects=True),
    )(examples, labels.reshape(1, rows))
    return z.reshape(width), w.reshape(1, width), u.reshape(1, width)


def solution(mesh):
    placed = (P(("grp", "dev"), None), P(("grp", "dev")))
    return jax.shard_map(
        functools.partial(per_device, mesh.shape["grp"], mesh.shape["dev"]),
        mesh=mesh,
        in_specs=placed,
        out_specs=(P(), P(("grp", "dev"), None), P(("grp", "dev"), None)),
        check_vma=False,
    )
```

```python
import functools

import jax
import jax.numpy as jnp
from jax import lax
from jax.experimental import pallas as pl
from jax.experimental.pallas import tpu as pltpu
from jax.sharding import PartitionSpec as P

PROX = 3
ROUNDS = 4
step_size = 200.0
penalty = 0.005
thresh = 0.04
shrinkage = 1.0 + step_size * penalty

LANES = 128
SUB = 8
GROUP = LANES * SUB
MESH = pl.DeviceIdType.MESH


def shrink(values):
    return values - jnp.clip(values, -thresh, thresh)


def kernel(
    n_grp, n_dev, cores,
    x_hbm, labels_ref,
    mean_out, comb_out, u_out,
    x, w, u, v, comb, arrived, partial, zfull,
    load_sem, rs_send, rs_recv, line_send, line_recv, ag_send, ag_recv, out_sem,
):
    rows = x.shape[1]
    blocks = x.shape[0]
    plane = n_grp * cores
    line = n_dev // cores
    per = blocks // plane
    members = n_grp * n_dev

    grp = lax.axis_index("grp")
    dev = lax.axis_index("dev")
    core = lax.rem(dev, cores)
    depth = lax.div(dev, cores)
    own = grp * cores + core

    def plane_peer(offset):
        a, b = offset // cores, offset % cores
        other_grp = lax.rem(grp + a, n_grp)
        other_core = lax.rem(core + b, cores)
        return (other_grp, depth * cores + other_core), other_grp * cores + other_core

    def line_peer(offset):
        return (grp, lax.rem(depth + offset, line) * cores + core)

    def load(i):
        return pltpu.make_async_copy(
            x_hbm.at[:, pl.ds(pl.multiple_of(i * GROUP, GROUP), GROUP)], x.at[i], load_sem.at[i]
        )

    def start_load(i, carry):
        load(i).start()
        return carry

    lax.fori_loop(0, blocks, start_load, 0)

    barrier = pltpu.get_barrier_semaphore()
    for offset in range(1, plane):
        pl.semaphore_signal(barrier, inc=1, device_id=plane_peer(offset)[0], device_id_type=MESH)
    for offset in range(1, line):
        pl.semaphore_signal(barrier, inc=1, device_id=line_peer(offset), device_id_type=MESH)

    eye = (
        lax.broadcasted_iota(jnp.int32, (rows, rows), 0) == lax.broadcasted_iota(jnp.int32, (rows, rows), 1)
    ).astype(jnp.float32)
    targets = jnp.sum(eye * labels_ref[...].astype(jnp.float32), axis=1, keepdims=True)

    for ref in (w, u, v):
        ref[...] = jnp.zeros_like(ref)

    def gram_block(step, total):
        for part in range(batch):
            i = step * batch + part
            load(i).wait()
            value = x[i]
            high = value.astype(jnp.bfloat16)
            low = (value - high.astype(jnp.float32)).astype(jnp.bfloat16)
            total = total + lax.dot_general(
                jnp.concatenate([high, low], axis=0), high, (((1,), (1,)), ((), ())), preferred_element_type=jnp.float32
            )
        return total

    batch = 16
    pairs = lax.fori_loop(0, blocks // batch, gram_block, jnp.zeros((2 * rows, rows), jnp.float32))
    mixed = pairs[rows:]
    g = pairs[:rows] + (mixed + mixed.T)

    pl.semaphore_wait(barrier, plane - 1 + line - 1)

    def rs_copy(t, offset):
        device, chunk = plane_peer(offset)
        return pltpu.make_async_remote_copy(
            src_ref=comb.at[pl.ds(chunk * per, per)],
            dst_ref=arrived.at[t, offset - 1],
            send_sem=rs_send.at[t, offset - 1],
            recv_sem=rs_recv.at[t, offset - 1],
            device_id=device,
            device_id_type=MESH,
        )

    def line_copy(t, offset):
        return pltpu.make_async_remote_copy(
            src_ref=partial.at[t, depth],
            dst_ref=partial.at[t, depth],
            send_sem=line_send.at[t, offset - 1],
            recv_sem=line_recv.at[t, offset - 1],
            device_id=line_peer(offset),
            device_id_type=MESH,
        )

    def ag_copy(t, offset):
        device, _ = plane_peer(offset)
        return pltpu.make_async_remote_copy(
            src_ref=zfull.at[t, pl.ds(own * per, per)],
            dst_ref=zfull.at[t, pl.ds(own * per, per)],
            send_sem=ag_send.at[t, offset - 1],
            recv_sem=ag_recv.at[t, offset - 1],
            device_id=device,
            device_id_type=MESH,
        )

    def local_steps(xw, xv):
        total = jnp.zeros_like(xw)
        for prox_index in range(PROX):
            residual = jax.nn.sigmoid(xw) - targets
            across = jnp.sum(eye * residual, axis=0, keepdims=True)
            gr = jnp.sum(g * across, axis=1, keepdims=True)
            xw = (xw - step_size * gr + step_size * penalty * xv) / shrinkage
            total = (total + step_size * residual) / shrinkage
        return xw, total

    w_keep = 1.0 / shrinkage**PROX
    v_gain = step_size * penalty * sum(1.0 / shrinkage ** (k + 1) for k in range(PROX))

    def weights_of(chunk, spread):
        def block(j, carry):
            i = chunk * per + j
            sums = []
            for lane in range(SUB):
                cols = slice(lane * LANES, (lane + 1) * LANES)
                acc = x[i, 0:SUB, cols] * spread[0:SUB]
                for k in range(SUB, rows, SUB):
                    acc += x[i, k : k + SUB, cols] * spread[k : k + SUB]
                sums.append(jnp.sum(acc, axis=0, keepdims=True))
            gradient = jnp.concatenate(sums, axis=0)
            fresh = w_keep * w[i] + v_gain * v[i] - gradient
            w[i] = fresh
            comb[i] = fresh + u[i]
            return carry

        lax.fori_loop(0, per, block, 0)

    def margins_of(t, chunk, accs):
        def block(j, accs):
            i = chunk * per + j
            out = list(accs)
            z = zfull[t, i]
            fresh = comb[i] - z
            u[i] = fresh
            v[i] = z - fresh
            for lane in range(SUB):
                cols = slice(lane * LANES, (lane + 1) * LANES)
                row = jnp.broadcast_to(z[lane : lane + 1], (SUB, LANES))
                for k in range(rows // SUB):
                    out[k] = out[k] + x[i, k * SUB : (k + 1) * SUB, cols] * row
            return tuple(out)

        return lax.fori_loop(0, per, block, accs)

    order = list(range(plane - 1, 0, -1))

    def reduce_round(t, total, point):
        spread = jnp.broadcast_to(total, (rows, LANES))
        for offset in order:
            weights_of(plane_peer(offset)[1], spread)
            rs_copy(t, offset).start()
        weights_of(own, spread)
        mine = comb[pl.ds(own * per, per)]
        for offset in order[::-1]:
            rs_copy(t, offset).wait_recv()
            mine = mine + arrived[t, offset - 1]
        partial[t, depth] = mine
        for offset in range(1, line):
            line_copy(t, offset).start()
        for offset in range(1, line):
            line_copy(t, offset).wait_recv()
        a = partial[t, 0]
        for k in range(1, line):
            a = a + partial[t, k]
        a = a * (1.0 / members) if members & (members - 1) == 0 else a / members
        zfull[t, pl.ds(own * per, per)] = point(a)
        for offset in order:
            ag_copy(t, offset).start()

    def sends_done(t):
        for offset in range(1, plane):
            rs_copy(t, offset).wait_send()
            ag_copy(t, offset).wait_send()
        for offset in range(1, line):
            line_copy(t, offset).wait_send()

    def source(offset):
        a, b = offset // cores, offset % cores
        return lax.rem(grp + n_grp - a, n_grp) * cores + lax.rem(core + cores - b, cores)

    def one_round(t, carried):
        xw, xu, xz = carried
        xw, total = local_steps(xw, xz - xu)
        reduce_round(t, total, shrink)
        accs = tuple(jnp.zeros((SUB, LANES), jnp.float32) for _ in range(rows // SUB))
        accs = margins_of(t, own, accs)
        for offset in order[::-1]:
            ag_copy(t, offset).wait_recv()
            accs = margins_of(t, source(offset), accs)
        fresh_xz = jnp.sum(jnp.concatenate(accs, axis=0), axis=1, keepdims=True)
        sends_done(t)
        return xw, xu + xw - fresh_xz, fresh_xz

    zero = jnp.zeros((rows, 1), jnp.float32)
    xw, xu, xz = lax.fori_loop(0, ROUNDS - 1, one_round, (zero, zero, zero))

    last = ROUNDS - 1
    _, total = local_steps(xw, xz - xu)
    u_copy = pltpu.make_async_copy(u, u_out, out_sem.at[plane])
    u_copy.start()
    reduce_round(last, total, lambda a: a)
    comb_copy = pltpu.make_async_copy(comb, comb_out, out_sem.at[plane + 1])
    comb_copy.start()

    def finish(chunk, slot):
        span = pl.ds(chunk * per, per)
        copy = pltpu.make_async_copy(zfull.at[last, span], mean_out.at[span], out_sem.at[slot])
        copy.start()
        return copy

    pending = [u_copy, comb_copy, finish(own, 0)]
    for offset in order[::-1]:
        ag_copy(last, offset).wait_recv()
        pending.append(finish(source(offset), offset))
    sends_done(last)
    for copy in pending:
        copy.wait()


def per_device(n_grp, n_dev, examples, labels):
    rows, width = examples.shape
    cores = 2 if n_dev % 2 == 0 else 1
    plane, line = n_grp * cores, n_dev // cores
    blocks = width // GROUP
    per = blocks // plane
    vector = jax.ShapeDtypeStruct((blocks, SUB, LANES), jnp.float32)
    anywhere = pl.BlockSpec(memory_space=pltpu.HBM)
    vec = pltpu.VMEM((blocks, SUB, LANES), jnp.float32)
    dma = pltpu.SemaphoreType.DMA
    mean, comb, old_u = pl.pallas_call(
        functools.partial(kernel, n_grp, n_dev, cores),
        out_shape=(vector, vector, vector),
        in_specs=[anywhere, pl.BlockSpec(memory_space=pltpu.VMEM)],
        out_specs=(anywhere, anywhere, anywhere),
        scratch_shapes=[
            pltpu.VMEM((blocks, rows, GROUP), jnp.float32),
            vec, vec, vec, vec,
            pltpu.VMEM((ROUNDS, plane - 1, per, SUB, LANES), jnp.float32),
            pltpu.VMEM((ROUNDS, line, per, SUB, LANES), jnp.float32),
            pltpu.VMEM((ROUNDS, blocks, SUB, LANES), jnp.float32),
            dma((blocks,)),
            dma((ROUNDS, plane - 1)), dma((ROUNDS, plane - 1)),
            dma((ROUNDS, line - 1)), dma((ROUNDS, line - 1)),
            dma((ROUNDS, plane - 1)), dma((ROUNDS, plane - 1)),
            dma((plane + 2,)),
        ],
        compiler_params=pltpu.CompilerParams(collective_id=0, has_side_effects=True),
    )(examples, labels.reshape(1, rows))
    z = shrink(mean)
    return z.reshape(width), (comb - old_u).reshape(1, width), (comb - z).reshape(1, width)


def solution(mesh):
    placed = (P(("grp", "dev"), None), P(("grp", "dev")))
    return jax.shard_map(
        functools.partial(per_device, mesh.shape["grp"], mesh.shape["dev"]),
        mesh=mesh,
        in_specs=placed,
        out_specs=(P(), P(("grp", "dev"), None), P(("grp", "dev"), None)),
        check_vma=False,
    )
```

```python
import functools

import jax
import jax.numpy as jnp
from jax import lax
from jax.experimental import pallas as pl
from jax.experimental.pallas import tpu as pltpu
from jax.sharding import PartitionSpec as P

PROX = 3
PARTS = 2
ROUNDS = 4
step_size = 200.0
penalty = 0.005
thresh = 0.04
shrinkage = 1.0 + step_size * penalty

LANES = 128
SUB = 8
GROUP = LANES * SUB
MESH = pl.DeviceIdType.MESH


def shrink(values):
    return values - jnp.clip(values, -thresh, thresh)


def kernel(
    n_grp, n_dev, cores, parts,
    x_hbm, labels_ref,
    mean_out, comb_out, u_out,
    x, w, u, v, comb, arrived, partial, zfull,
    load_sem, rs_send, rs_recv, line_send, line_recv, ag_send, ag_recv, out_sem,
):
    rows = x.shape[1]
    blocks = x.shape[0]
    plane = n_grp * cores
    line = n_dev // cores
    per = blocks // plane
    piece = per // parts
    members = n_grp * n_dev

    grp = lax.axis_index("grp")
    dev = lax.axis_index("dev")
    core = lax.rem(dev, cores)
    depth = lax.div(dev, cores)
    own = grp * cores + core

    def shift(position, size, offset):
        if size % 2:
            return lax.rem(position + (offset + size) % size, size)
        half = size // 2
        high = lax.rem(lax.div(position, 2) + (offset // 2 if offset > 0 else half - (-offset) // 2), half)
        return high * 2 + lax.rem(position + abs(offset) % 2, 2)

    def plane_member(offset, sign):
        return shift(grp, n_grp, sign * (offset // cores)), lax.rem(core + offset % cores, cores)

    def plane_peer(offset):
        other_grp, other_core = plane_member(offset, 1)
        return (other_grp, depth * cores + other_core), other_grp * cores + other_core

    def source(offset):
        other_grp, other_core = plane_member(offset, -1)
        return other_grp * cores + other_core

    def line_peer(offset):
        return (grp, shift(depth, line, offset) * cores + core)

    def load(i):
        return pltpu.make_async_copy(
            x_hbm.at[:, pl.ds(pl.multiple_of(i * GROUP, GROUP), GROUP)], x.at[i], load_sem.at[i]
        )

    def start_load(i, carry):
        load(i).start()
        return carry

    lax.fori_loop(0, blocks, start_load, 0)

    barrier = pltpu.get_barrier_semaphore()
    for offset in range(1, plane):
        pl.semaphore_signal(barrier, inc=1, device_id=plane_peer(offset)[0], device_id_type=MESH)
    for offset in range(1, line):
        pl.semaphore_signal(barrier, inc=1, device_id=line_peer(offset), device_id_type=MESH)

    eye = (
        lax.broadcasted_iota(jnp.int32, (rows, rows), 0) == lax.broadcasted_iota(jnp.int32, (rows, rows), 1)
    ).astype(jnp.float32)
    across = labels_ref[...].astype(jnp.float32)
    targets = jnp.sum(eye * across, axis=1, keepdims=True), across

    for ref in (w, u, v):
        ref[...] = jnp.zeros_like(ref)

    def gram_block(step, total):
        for part in range(batch):
            i = step * batch + part
            load(i).wait()
            value = x[i]
            high = value.astype(jnp.bfloat16)
            low = (value - high.astype(jnp.float32)).astype(jnp.bfloat16)
            total = total + lax.dot_general(
                jnp.concatenate([high, low], axis=0), high, (((1,), (1,)), ((), ())), preferred_element_type=jnp.float32
            )
        return total

    batch = 16
    pairs = lax.fori_loop(0, blocks // batch, gram_block, jnp.zeros((2 * rows, rows), jnp.float32))
    mixed = pairs[rows:]
    g = pairs[:rows] + (mixed + mixed.T)

    pl.semaphore_wait(barrier, plane - 1 + line - 1)

    def rs_copy(t, h, offset):
        device, chunk = plane_peer(offset)
        return pltpu.make_async_remote_copy(
            src_ref=comb.at[pl.ds(chunk * per + h * piece, piece)],
            dst_ref=arrived.at[t, h, offset - 1],
            send_sem=rs_send.at[t, h, offset - 1],
            recv_sem=rs_recv.at[t, h, offset - 1],
            device_id=device,
            device_id_type=MESH,
        )

    def line_copy(t, h, offset):
        return pltpu.make_async_remote_copy(
            src_ref=partial.at[t, h, depth],
            dst_ref=partial.at[t, h, depth],
            send_sem=line_send.at[t, h, offset - 1],
            recv_sem=line_recv.at[t, h, offset - 1],
            device_id=line_peer(offset),
            device_id_type=MESH,
        )

    def ag_copy(t, h, offset):
        device, _ = plane_peer(offset)
        span = pl.ds(own * per + h * piece, piece)
        return pltpu.make_async_remote_copy(
            src_ref=zfull.at[t, span],
            dst_ref=zfull.at[t, span],
            send_sem=ag_send.at[t, h, offset - 1],
            recv_sem=ag_recv.at[t, h, offset - 1],
            device_id=device,
            device_id_type=MESH,
        )

    def turned(value, axis):
        return jnp.sum(eye * value, axis=axis, keepdims=True)

    def local_steps(xw, xv):
        total = jnp.zeros_like(xw)
        both_xv = xv, turned(xv, 0)
        for prox_index in range(PROX - 1):
            axis = prox_index % 2
            residual = jax.nn.sigmoid(xw) - targets[axis]
            moved = jnp.sum(eye * xw - step_size * (g * residual), axis=axis, keepdims=True)
            xw = (moved + step_size * penalty * both_xv[1 - axis]) / shrinkage
            total = (total + step_size * (turned(residual, 1) if axis else residual)) / shrinkage
        if PROX % 2 == 0:
            xw = turned(xw, 1)
        residual = jax.nn.sigmoid(xw) - targets[0]
        total = (total + step_size * residual) / shrinkage

        def finish_step():
            moved = jnp.sum(g * turned(residual, 0), axis=1, keepdims=True)
            return (xw - step_size * moved + step_size * penalty * xv) / shrinkage

        return finish_step, total

    w_keep = 1.0 / shrinkage**PROX
    v_gain = step_size * penalty * sum(1.0 / shrinkage ** (k + 1) for k in range(PROX))

    def weights_of(chunk, h, spread):
        def block(j, carry):
            i = chunk * per + h * piece + j
            sums = []
            for lane in range(SUB):
                cols = slice(lane * LANES, (lane + 1) * LANES)
                acc = x[i, 0:SUB, cols] * spread[0:SUB]
                for k in range(SUB, rows, SUB):
                    acc += x[i, k : k + SUB, cols] * spread[k : k + SUB]
                sums.append(jnp.sum(acc, axis=0, keepdims=True))
            gradient = jnp.concatenate(sums, axis=0)
            fresh = w_keep * w[i] + v_gain * v[i] - gradient
            w[i] = fresh
            comb[i] = fresh + u[i]
            return carry

        lax.fori_loop(0, piece, block, 0)

    def margins_of(t, chunk, h, accs):
        def block(j, accs):
            i = chunk * per + h * piece + j
            out = list(accs)
            z = zfull[t, i]
            fresh = comb[i] - z
            u[i] = fresh
            v[i] = z - fresh
            for lane in range(SUB):
                cols = slice(lane * LANES, (lane + 1) * LANES)
                row = jnp.broadcast_to(z[lane : lane + 1], (SUB, LANES))
                for k in range(rows // SUB):
                    out[k] = out[k] + x[i, k * SUB : (k + 1) * SUB, cols] * row
            return tuple(out)

        return lax.fori_loop(0, piece, block, accs)

    order = list(range(plane - 1, 0, -1))

    def reduce_round(t, total, point):
        spread = jnp.broadcast_to(total, (rows, LANES))
        for h in range(parts):
            for offset in order:
                weights_of(plane_peer(offset)[1], h, spread)
                rs_copy(t, h, offset).start()
        for h in range(parts):
            weights_of(own, h, spread)
        for h in range(parts):
            mine = comb[pl.ds(own * per + h * piece, piece)]
            for offset in order[::-1]:
                rs_copy(t, h, offset).wait_recv()
                mine = mine + arrived[t, h, offset - 1]
            partial[t, h, depth] = mine
            for offset in range(line - 1, 0, -1):
                line_copy(t, h, offset).start()
        for h in range(parts):
            for offset in range(1, line):
                line_copy(t, h, offset).wait_recv()
            a = partial[t, h, 0]
            for k in range(1, line):
                a = a + partial[t, h, k]
            a = a * (1.0 / members) if members & (members - 1) == 0 else a / members
            zfull[t, pl.ds(own * per + h * piece, piece)] = point(a)
            for offset in order:
                ag_copy(t, h, offset).start()

    def sends_done(t):
        for h in range(parts):
            for offset in range(1, plane):
                rs_copy(t, h, offset).wait_send()
                ag_copy(t, h, offset).wait_send()
            for offset in range(1, line):
                line_copy(t, h, offset).wait_send()

    def one_round(t, carried):
        xw, xu, xz = carried
        finish_step, total = local_steps(xw, xz - xu)
        reduce_round(t, total, shrink)
        xw = finish_step()
        accs = tuple(jnp.zeros((SUB, LANES), jnp.float32) for _ in range(rows // SUB))
        for h in range(parts):
            accs = margins_of(t, own, h, accs)
        for h in range(parts):
            for offset in order[::-1]:
                ag_copy(t, h, offset).wait_recv()
                accs = margins_of(t, source(offset), h, accs)
        fresh_xz = jnp.sum(jnp.concatenate(accs, axis=0), axis=1, keepdims=True)
        sends_done(t)
        return xw, xu + xw - fresh_xz, fresh_xz

    zero = jnp.zeros((rows, 1), jnp.float32)
    xw, xu, xz = lax.fori_loop(0, ROUNDS - 1, one_round, (zero, zero, zero))

    last = ROUNDS - 1
    _, total = local_steps(xw, xz - xu)
    u_copy = pltpu.make_async_copy(u, u_out, out_sem.at[plane])
    u_copy.start()
    reduce_round(last, total, lambda a: a)
    comb_copy = pltpu.make_async_copy(comb, comb_out, out_sem.at[plane + 1])
    comb_copy.start()

    def finish(chunk, slot):
        span = pl.ds(chunk * per, per)
        copy = pltpu.make_async_copy(zfull.at[last, span], mean_out.at[span], out_sem.at[slot])
        copy.start()
        return copy

    pending = [u_copy, comb_copy, finish(own, 0)]
    for offset in order[::-1]:
        for h in range(parts):
            ag_copy(last, h, offset).wait_recv()
        pending.append(finish(source(offset), offset))
    sends_done(last)
    for copy in pending:
        copy.wait()


def per_device(n_grp, n_dev, examples, labels):
    rows, width = examples.shape
    cores = 2 if n_dev % 2 == 0 else 1
    plane, line = n_grp * cores, n_dev // cores
    blocks = width // GROUP
    per = blocks // plane
    parts = PARTS if per % PARTS == 0 else 1
    vector = jax.ShapeDtypeStruct((blocks, SUB, LANES), jnp.float32)
    anywhere = pl.BlockSpec(memory_space=pltpu.HBM)
    vec = pltpu.VMEM((blocks, SUB, LANES), jnp.float32)
    dma = pltpu.SemaphoreType.DMA
    mean, comb, old_u = pl.pallas_call(
        functools.partial(kernel, n_grp, n_dev, cores, parts),
        out_shape=(vector, vector, vector),
        in_specs=[anywhere, pl.BlockSpec(memory_space=pltpu.VMEM)],
        out_specs=(anywhere, anywhere, anywhere),
        scratch_shapes=[
            pltpu.VMEM((blocks, rows, GROUP), jnp.float32),
            vec, vec, vec, vec,
            pltpu.VMEM((ROUNDS, parts, plane - 1, per // parts, SUB, LANES), jnp.float32),
            pltpu.VMEM((ROUNDS, parts, line, per // parts, SUB, LANES), jnp.float32),
            pltpu.VMEM((ROUNDS, blocks, SUB, LANES), jnp.float32),
            dma((blocks,)),
            dma((ROUNDS, parts, plane - 1)), dma((ROUNDS, parts, plane - 1)),
            dma((ROUNDS, parts, line - 1)), dma((ROUNDS, parts, line - 1)),
            dma((ROUNDS, parts, plane - 1)), dma((ROUNDS, parts, plane - 1)),
            dma((plane + 2,)),
        ],
        compiler_params=pltpu.CompilerParams(collective_id=0, has_side_effects=True),
    )(examples, labels.reshape(1, rows))
    z = shrink(mean)
    return z.reshape(width), (comb - old_u).reshape(1, width), (comb - z).reshape(1, width)


def solution(mesh):
    placed = (P(("grp", "dev"), None), P(("grp", "dev")))
    return jax.shard_map(
        functools.partial(per_device, mesh.shape["grp"], mesh.shape["dev"]),
        mesh=mesh,
        in_specs=placed,
        out_specs=(P(), P(("grp", "dev"), None), P(("grp", "dev"), None)),
        check_vma=False,
    )
```

```python
import functools

import jax
import jax.numpy as jnp
from jax import lax
from jax.experimental import pallas as pl
from jax.experimental.pallas import tpu as pltpu
from jax.sharding import PartitionSpec as P

PROX = 3
PARTS = 2
ROUNDS = 4
step_size = 200.0
penalty = 0.005
thresh = 0.04
shrinkage = 1.0 + step_size * penalty

LANES = 128
SUB = 8
GROUP = LANES * SUB
MESH = pl.DeviceIdType.MESH


def shrink(values):
    return values - jnp.clip(values, -thresh, thresh)


def kernel(
    n_grp, n_dev, cores, parts,
    x_hbm, labels_ref,
    mean_out, comb_out, u_out,
    x, w, u, v, comb, arrived, partial, zfull,
    load_sem, rs_send, rs_recv, line_send, line_recv, ag_send, ag_recv, out_sem,
):
    rows = x.shape[1]
    blocks = x.shape[0]
    plane = n_grp * cores
    line = n_dev // cores
    per = blocks // plane
    piece = per // parts
    members = n_grp * n_dev

    grp = lax.axis_index("grp")
    dev = lax.axis_index("dev")
    core = lax.rem(dev, cores)
    depth = lax.div(dev, cores)
    own = grp * cores + core

    def shift(position, size, offset):
        if size % 2:
            return lax.rem(position + (offset + size) % size, size)
        half = size // 2
        high = lax.rem(lax.div(position, 2) + (offset // 2 if offset > 0 else half - (-offset) // 2), half)
        return high * 2 + lax.rem(position + abs(offset) % 2, 2)

    def plane_member(offset, sign):
        return shift(grp, n_grp, sign * (offset // cores)), lax.rem(core + offset % cores, cores)

    def plane_peer(offset):
        other_grp, other_core = plane_member(offset, 1)
        return (other_grp, depth * cores + other_core), other_grp * cores + other_core

    def source(offset):
        other_grp, other_core = plane_member(offset, -1)
        return other_grp * cores + other_core

    def line_peer(offset):
        return (grp, shift(depth, line, offset) * cores + core)

    def load(i):
        return pltpu.make_async_copy(
            x_hbm.at[:, pl.ds(pl.multiple_of(i * GROUP, GROUP), GROUP)], x.at[i], load_sem.at[i]
        )

    def start_load(i, carry):
        load(i).start()
        return carry

    lax.fori_loop(0, blocks, start_load, 0)

    barrier = pltpu.get_barrier_semaphore()
    for offset in range(1, plane):
        pl.semaphore_signal(barrier, inc=1, device_id=plane_peer(offset)[0], device_id_type=MESH)
    for offset in range(1, line):
        pl.semaphore_signal(barrier, inc=1, device_id=line_peer(offset), device_id_type=MESH)

    eye = (
        lax.broadcasted_iota(jnp.int32, (rows, rows), 0) == lax.broadcasted_iota(jnp.int32, (rows, rows), 1)
    ).astype(jnp.float32)
    across = labels_ref[...].astype(jnp.float32)
    targets = jnp.sum(eye * across, axis=1, keepdims=True), across

    for ref in (w, u, v):
        ref[...] = jnp.zeros_like(ref)

    def gram_block(step, total):
        for part in range(batch):
            i = step * batch + part
            load(i).wait()
            value = x[i]
            high = value.astype(jnp.bfloat16)
            low = (value - high.astype(jnp.float32)).astype(jnp.bfloat16)
            total = total + lax.dot_general(
                jnp.concatenate([high, low], axis=0), high, (((1,), (1,)), ((), ())), preferred_element_type=jnp.float32
            )
        return total

    batch = 16
    pairs = lax.fori_loop(0, blocks // batch, gram_block, jnp.zeros((2 * rows, rows), jnp.float32))
    mixed = pairs[rows:]
    g = pairs[:rows] + (mixed + mixed.T)

    pl.semaphore_wait(barrier, plane - 1 + line - 1)

    def rs_copy(t, h, offset):
        device, chunk = plane_peer(offset)
        return pltpu.make_async_remote_copy(
            src_ref=comb.at[pl.ds(chunk * per + h * piece, piece)],
            dst_ref=arrived.at[t, h, offset - 1],
            send_sem=rs_send.at[t, h, offset - 1],
            recv_sem=rs_recv.at[t, h, offset - 1],
            device_id=device,
            device_id_type=MESH,
        )

    def line_copy(t, h, offset):
        return pltpu.make_async_remote_copy(
            src_ref=partial.at[t, h, depth],
            dst_ref=partial.at[t, h, depth],
            send_sem=line_send.at[t, h, offset - 1],
            recv_sem=line_recv.at[t, h, offset - 1],
            device_id=line_peer(offset),
            device_id_type=MESH,
        )

    def ag_copy(t, h, offset):
        device, _ = plane_peer(offset)
        span = pl.ds(own * per + h * piece, piece)
        return pltpu.make_async_remote_copy(
            src_ref=zfull.at[t, span],
            dst_ref=zfull.at[t, span],
            send_sem=ag_send.at[t, h, offset - 1],
            recv_sem=ag_recv.at[t, h, offset - 1],
            device_id=device,
            device_id_type=MESH,
        )

    def turned(value, axis):
        return jnp.sum(eye * value, axis=axis, keepdims=True)

    def local_steps(xw, xv):
        total = jnp.zeros_like(xw)
        both_xv = xv, turned(xv, 0)
        for prox_index in range(PROX - 1):
            axis = prox_index % 2
            residual = jax.nn.sigmoid(xw) - targets[axis]
            moved = jnp.sum(eye * xw - step_size * (g * residual), axis=axis, keepdims=True)
            xw = (moved + step_size * penalty * both_xv[1 - axis]) / shrinkage
            total = (total + step_size * (turned(residual, 1) if axis else residual)) / shrinkage
        if PROX % 2 == 0:
            xw = turned(xw, 1)
        residual = jax.nn.sigmoid(xw) - targets[0]
        total = (total + step_size * residual) / shrinkage

        def finish_step():
            moved = jnp.sum(g * turned(residual, 0), axis=1, keepdims=True)
            return (xw - step_size * moved + step_size * penalty * xv) / shrinkage

        return finish_step, total

    w_keep = 1.0 / shrinkage**PROX
    v_gain = step_size * penalty * sum(1.0 / shrinkage ** (k + 1) for k in range(PROX))

    def weights_of(chunk, h, spread):
        def block(j, carry):
            i = chunk * per + h * piece + j
            sums = []
            for lane in range(SUB):
                cols = slice(lane * LANES, (lane + 1) * LANES)
                acc = x[i, 0:SUB, cols] * spread[0:SUB]
                for k in range(SUB, rows, SUB):
                    acc += x[i, k : k + SUB, cols] * spread[k : k + SUB]
                sums.append(jnp.sum(acc, axis=0, keepdims=True))
            gradient = jnp.concatenate(sums, axis=0)
            fresh = w_keep * w[i] + v_gain * v[i] - gradient
            w[i] = fresh
            comb[i] = fresh + u[i]
            return carry

        lax.fori_loop(0, piece, block, 0, unroll=True)

    def margins_of(t, chunk, h, accs):
        def block(j, accs):
            i = chunk * per + h * piece + j
            out = list(accs)
            z = zfull[t, i]
            fresh = comb[i] - z
            u[i] = fresh
            v[i] = z - fresh
            for lane in range(SUB):
                cols = slice(lane * LANES, (lane + 1) * LANES)
                row = jnp.broadcast_to(z[lane : lane + 1], (SUB, LANES))
                for k in range(rows // SUB):
                    out[k] = out[k] + x[i, k * SUB : (k + 1) * SUB, cols] * row
            return tuple(out)

        return lax.fori_loop(0, piece, block, accs, unroll=True)

    order = list(range(plane - 1, 0, -1))

    def reduce_round(t, total, point):
        spread = jnp.broadcast_to(total, (rows, LANES))
        for h in range(parts):
            for offset in order:
                weights_of(plane_peer(offset)[1], h, spread)
                rs_copy(t, h, offset).start()
        for h in range(parts):
            weights_of(own, h, spread)
        for h in range(parts):
            mine = comb[pl.ds(own * per + h * piece, piece)]
            for offset in order[::-1]:
                rs_copy(t, h, offset).wait_recv()
                mine = mine + arrived[t, h, offset - 1]
            partial[t, h, depth] = mine
            for offset in range(line - 1, 0, -1):
                line_copy(t, h, offset).start()
        for h in range(parts):
            for offset in range(1, line):
                line_copy(t, h, offset).wait_recv()
            a = partial[t, h, 0]
            for k in range(1, line):
                a = a + partial[t, h, k]
            a = a * (1.0 / members) if members & (members - 1) == 0 else a / members
            zfull[t, pl.ds(own * per + h * piece, piece)] = point(a)
            for offset in order:
                ag_copy(t, h, offset).start()

    def sends_done(t):
        for h in range(parts):
            for offset in range(1, plane):
                rs_copy(t, h, offset).wait_send()
                ag_copy(t, h, offset).wait_send()
            for offset in range(1, line):
                line_copy(t, h, offset).wait_send()

    def one_round(t, carried):
        xw, xu, xz = carried
        finish_step, total = local_steps(xw, xz - xu)
        reduce_round(t, total, shrink)
        xw = finish_step()
        accs = tuple(jnp.zeros((SUB, LANES), jnp.float32) for _ in range(rows // SUB))
        for h in range(parts):
            accs = margins_of(t, own, h, accs)
        for h in range(parts):
            for offset in order[::-1]:
                ag_copy(t, h, offset).wait_recv()
                accs = margins_of(t, source(offset), h, accs)
        fresh_xz = jnp.sum(jnp.concatenate(accs, axis=0), axis=1, keepdims=True)
        sends_done(t)
        return xw, xu + xw - fresh_xz, fresh_xz

    zero = jnp.zeros((rows, 1), jnp.float32)
    xw, xu, xz = lax.fori_loop(0, ROUNDS - 1, one_round, (zero, zero, zero))

    last = ROUNDS - 1
    _, total = local_steps(xw, xz - xu)
    u_copy = pltpu.make_async_copy(u, u_out, out_sem.at[plane])
    u_copy.start()
    reduce_round(last, total, lambda a: a)
    comb_copy = pltpu.make_async_copy(comb, comb_out, out_sem.at[plane + 1])
    comb_copy.start()

    def finish(chunk, slot):
        span = pl.ds(chunk * per, per)
        copy = pltpu.make_async_copy(zfull.at[last, span], mean_out.at[span], out_sem.at[slot])
        copy.start()
        return copy

    pending = [u_copy, comb_copy, finish(own, 0)]
    for offset in order[::-1]:
        for h in range(parts):
            ag_copy(last, h, offset).wait_recv()
        pending.append(finish(source(offset), offset))
    sends_done(last)
    for copy in pending:
        copy.wait()


def per_device(n_grp, n_dev, examples, labels):
    rows, width = examples.shape
    cores = 2 if n_dev % 2 == 0 else 1
    plane, line = n_grp * cores, n_dev // cores
    blocks = width // GROUP
    per = blocks // plane
    parts = PARTS if per % PARTS == 0 else 1
    vector = jax.ShapeDtypeStruct((blocks, SUB, LANES), jnp.float32)
    anywhere = pl.BlockSpec(memory_space=pltpu.HBM)
    vec = pltpu.VMEM((blocks, SUB, LANES), jnp.float32)
    dma = pltpu.SemaphoreType.DMA
    mean, comb, old_u = pl.pallas_call(
        functools.partial(kernel, n_grp, n_dev, cores, parts),
        out_shape=(vector, vector, vector),
        in_specs=[anywhere, pl.BlockSpec(memory_space=pltpu.VMEM)],
        out_specs=(anywhere, anywhere, anywhere),
        scratch_shapes=[
            pltpu.VMEM((blocks, rows, GROUP), jnp.float32),
            vec, vec, vec, vec,
            pltpu.VMEM((ROUNDS, parts, plane - 1, per // parts, SUB, LANES), jnp.float32),
            pltpu.VMEM((ROUNDS, parts, line, per // parts, SUB, LANES), jnp.float32),
            pltpu.VMEM((ROUNDS, blocks, SUB, LANES), jnp.float32),
            dma((blocks,)),
            dma((ROUNDS, parts, plane - 1)), dma((ROUNDS, parts, plane - 1)),
            dma((ROUNDS, parts, line - 1)), dma((ROUNDS, parts, line - 1)),
            dma((ROUNDS, parts, plane - 1)), dma((ROUNDS, parts, plane - 1)),
            dma((plane + 2,)),
        ],
        compiler_params=pltpu.CompilerParams(collective_id=0, has_side_effects=True),
    )(examples, labels.reshape(1, rows))
    z = shrink(mean)
    return z.reshape(width), (comb - old_u).reshape(1, width), (comb - z).reshape(1, width)


def solution(mesh):
    placed = (P(("grp", "dev"), None), P(("grp", "dev")))
    return jax.shard_map(
        functools.partial(per_device, mesh.shape["grp"], mesh.shape["dev"]),
        mesh=mesh,
        in_specs=placed,
        out_specs=(P(), P(("grp", "dev"), None), P(("grp", "dev"), None)),
        check_vma=False,
    )
```

```python
import functools

import jax
import jax.numpy as jnp
from jax import lax
from jax.experimental import pallas as pl
from jax.experimental.pallas import tpu as pltpu
from jax.sharding import PartitionSpec as P

PROX = 3
PARTS = 2
ROUNDS = 4
step_size = 200.0
penalty = 0.005
thresh = 0.04
shrinkage = 1.0 + step_size * penalty

LANES = 128
SUB = 8
GROUP = LANES * SUB
MESH = pl.DeviceIdType.MESH


def shrink(values):
    return values - jnp.clip(values, -thresh, thresh)


def kernel(
    n_grp, n_dev, cores, parts,
    x_hbm, labels_ref,
    mean_out, comb_out, u_out,
    x, w, u, v, comb, arrived, partial, zfull,
    load_sem, rs_send, rs_recv, line_send, line_recv, ag_send, ag_recv, out_sem,
):
    rows = x.shape[1]
    blocks = x.shape[0]
    plane = n_grp * cores
    line = n_dev // cores
    per = blocks // plane
    piece = per // parts
    members = n_grp * n_dev

    grp = lax.axis_index("grp")
    dev = lax.axis_index("dev")
    core = lax.rem(dev, cores)
    depth = lax.div(dev, cores)
    own = grp * cores + core

    def shift(position, size, offset):
        if size % 2:
            return lax.rem(position + (offset + size) % size, size)
        half = size // 2
        high = lax.rem(lax.div(position, 2) + (offset // 2 if offset > 0 else half - (-offset) // 2), half)
        return high * 2 + lax.rem(position + abs(offset) % 2, 2)

    def plane_member(offset, sign):
        return shift(grp, n_grp, sign * (offset // cores)), lax.rem(core + offset % cores, cores)

    def plane_peer(offset):
        other_grp, other_core = plane_member(offset, 1)
        return (other_grp, depth * cores + other_core), other_grp * cores + other_core

    def source(offset):
        other_grp, other_core = plane_member(offset, -1)
        return other_grp * cores + other_core

    def line_peer(offset):
        return (grp, shift(depth, line, offset) * cores + core)

    def load(i):
        return pltpu.make_async_copy(
            x_hbm.at[:, pl.ds(pl.multiple_of(i * GROUP, GROUP), GROUP)], x.at[i], load_sem.at[i]
        )

    def start_load(i, carry):
        load(i).start()
        return carry

    lax.fori_loop(0, blocks, start_load, 0)

    barrier = pltpu.get_barrier_semaphore()
    for offset in range(1, plane):
        pl.semaphore_signal(barrier, inc=1, device_id=plane_peer(offset)[0], device_id_type=MESH)
    for offset in range(1, line):
        pl.semaphore_signal(barrier, inc=1, device_id=line_peer(offset), device_id_type=MESH)

    eye = (
        lax.broadcasted_iota(jnp.int32, (rows, rows), 0) == lax.broadcasted_iota(jnp.int32, (rows, rows), 1)
    ).astype(jnp.float32)
    across = labels_ref[...].astype(jnp.float32)
    targets = jnp.sum(eye * across, axis=1, keepdims=True), across

    for ref in (w, u, v):
        ref[...] = jnp.zeros_like(ref)

    def gram_block(step, total):
        for part in range(batch // 2):
            i = step * batch + part * 2
            load(i).wait()
            load(i + 1).wait()
            value = jnp.concatenate([x[i], x[i + 1]], axis=1)
            high = value.astype(jnp.bfloat16)
            low = (value - high.astype(jnp.float32)).astype(jnp.bfloat16)
            total = total + lax.dot_general(
                jnp.concatenate([high, low], axis=0), high, (((1,), (1,)), ((), ())), preferred_element_type=jnp.float32
            )
        return total

    batch = 16
    pairs = lax.fori_loop(0, blocks // batch, gram_block, jnp.zeros((2 * rows, rows), jnp.float32))
    mixed = pairs[rows:]
    g = pairs[:rows] + (mixed + mixed.T)

    pl.semaphore_wait(barrier, plane - 1 + line - 1)

    def rs_copy(t, h, offset):
        device, chunk = plane_peer(offset)
        return pltpu.make_async_remote_copy(
            src_ref=comb.at[pl.ds(chunk * per + h * piece, piece)],
            dst_ref=arrived.at[t, h, offset - 1],
            send_sem=rs_send.at[t, h, offset - 1],
            recv_sem=rs_recv.at[t, h, offset - 1],
            device_id=device,
            device_id_type=MESH,
        )

    def line_copy(t, h, offset):
        return pltpu.make_async_remote_copy(
            src_ref=partial.at[t, h, depth],
            dst_ref=partial.at[t, h, depth],
            send_sem=line_send.at[t, h, offset - 1],
            recv_sem=line_recv.at[t, h, offset - 1],
            device_id=line_peer(offset),
            device_id_type=MESH,
        )

    def ag_copy(t, h, offset):
        device, _ = plane_peer(offset)
        span = pl.ds(own * per + h * piece, piece)
        return pltpu.make_async_remote_copy(
            src_ref=zfull.at[t, span],
            dst_ref=zfull.at[t, span],
            send_sem=ag_send.at[t, h, offset - 1],
            recv_sem=ag_recv.at[t, h, offset - 1],
            device_id=device,
            device_id_type=MESH,
        )

    def turned(value, axis):
        return jnp.sum(eye * value, axis=axis, keepdims=True)

    def local_steps(xw, xv):
        total = jnp.zeros_like(xw)
        both_xv = xv, turned(xv, 0)
        for prox_index in range(PROX - 1):
            axis = prox_index % 2
            residual = jax.nn.sigmoid(xw) - targets[axis]
            moved = jnp.sum(eye * xw - step_size * (g * residual), axis=axis, keepdims=True)
            xw = (moved + step_size * penalty * both_xv[1 - axis]) / shrinkage
            total = (total + step_size * (turned(residual, 1) if axis else residual)) / shrinkage
        if PROX % 2 == 0:
            xw = turned(xw, 1)
        residual = jax.nn.sigmoid(xw) - targets[0]
        total = (total + step_size * residual) / shrinkage

        def finish_step():
            moved = jnp.sum(g * turned(residual, 0), axis=1, keepdims=True)
            return (xw - step_size * moved + step_size * penalty * xv) / shrinkage

        return finish_step, total

    w_keep = 1.0 / shrinkage**PROX
    v_gain = step_size * penalty * sum(1.0 / shrinkage ** (k + 1) for k in range(PROX))

    def weights_of(chunk, h, spread):
        def block(j, carry):
            i = chunk * per + h * piece + j
            sums = []
            for lane in range(SUB):
                cols = slice(lane * LANES, (lane + 1) * LANES)
                acc = x[i, 0:SUB, cols] * spread[0:SUB]
                for k in range(SUB, rows, SUB):
                    acc += x[i, k : k + SUB, cols] * spread[k : k + SUB]
                sums.append(jnp.sum(acc, axis=0, keepdims=True))
            gradient = jnp.concatenate(sums, axis=0)
            fresh = w_keep * w[i] + v_gain * v[i] - gradient
            w[i] = fresh
            comb[i] = fresh + u[i]
            return carry

        lax.fori_loop(0, piece, block, 0, unroll=True)

    def margins_of(t, chunk, h, accs):
        def block(j, accs):
            i = chunk * per + h * piece + j
            out = list(accs)
            z = zfull[t, i]
            fresh = comb[i] - z
            u[i] = fresh
            v[i] = z - fresh
            for lane in range(SUB):
                cols = slice(lane * LANES, (lane + 1) * LANES)
                row = jnp.broadcast_to(z[lane : lane + 1], (SUB, LANES))
                for k in range(rows // SUB):
                    out[k] = out[k] + x[i, k * SUB : (k + 1) * SUB, cols] * row
            return tuple(out)

        return lax.fori_loop(0, piece, block, accs, unroll=True)

    order = list(range(plane - 1, 0, -1))

    def reduce_round(t, total, point):
        spread = jnp.broadcast_to(total, (rows, LANES))
        for h in range(parts):
            for offset in order:
                weights_of(plane_peer(offset)[1], h, spread)
                rs_copy(t, h, offset).start()
        for h in range(parts):
            weights_of(own, h, spread)
            mine = comb[pl.ds(own * per + h * piece, piece)]
            for offset in order[::-1]:
                rs_copy(t, h, offset).wait_recv()
                mine = mine + arrived[t, h, offset - 1]
            partial[t, h, depth] = mine
            for offset in range(line - 1, 0, -1):
                line_copy(t, h, offset).start()
        for h in range(parts):
            for offset in range(1, line):
                line_copy(t, h, offset).wait_recv()
            a = partial[t, h, 0]
            for k in range(1, line):
                a = a + partial[t, h, k]
            a = a * (1.0 / members) if members & (members - 1) == 0 else a / members
            zfull[t, pl.ds(own * per + h * piece, piece)] = point(a)
            for offset in order:
                ag_copy(t, h, offset).start()

    def sends_done(t):
        for h in range(parts):
            for offset in range(1, plane):
                rs_copy(t, h, offset).wait_send()
                ag_copy(t, h, offset).wait_send()
            for offset in range(1, line):
                line_copy(t, h, offset).wait_send()

    def one_round(t, carried):
        xw, xu, xz = carried
        finish_step, total = local_steps(xw, xz - xu)
        reduce_round(t, total, shrink)
        xw = finish_step()
        accs = tuple(jnp.zeros((SUB, LANES), jnp.float32) for _ in range(rows // SUB))
        for h in range(parts):
            accs = margins_of(t, own, h, accs)
        for h in range(parts):
            for offset in order[::-1]:
                ag_copy(t, h, offset).wait_recv()
                accs = margins_of(t, source(offset), h, accs)
        fresh_xz = jnp.sum(jnp.concatenate(accs, axis=0), axis=1, keepdims=True)
        sends_done(t)
        return xw, xu + xw - fresh_xz, fresh_xz

    zero = jnp.zeros((rows, 1), jnp.float32)
    xw, xu, xz = lax.fori_loop(0, ROUNDS - 1, one_round, (zero, zero, zero))

    last = ROUNDS - 1
    _, total = local_steps(xw, xz - xu)
    u_copy = pltpu.make_async_copy(u, u_out, out_sem.at[plane])
    u_copy.start()
    reduce_round(last, total, lambda a: a)
    comb_copy = pltpu.make_async_copy(comb, comb_out, out_sem.at[plane + 1])
    comb_copy.start()

    def finish(chunk, slot):
        span = pl.ds(chunk * per, per)
        copy = pltpu.make_async_copy(zfull.at[last, span], mean_out.at[span], out_sem.at[slot])
        copy.start()
        return copy

    pending = [u_copy, comb_copy, finish(own, 0)]
    for offset in order[::-1]:
        for h in range(parts):
            ag_copy(last, h, offset).wait_recv()
        pending.append(finish(source(offset), offset))
    sends_done(last)
    for copy in pending:
        copy.wait()


def per_device(n_grp, n_dev, examples, labels):
    rows, width = examples.shape
    cores = 2 if n_dev % 2 == 0 else 1
    plane, line = n_grp * cores, n_dev // cores
    blocks = width // GROUP
    per = blocks // plane
    parts = PARTS if per % PARTS == 0 else 1
    vector = jax.ShapeDtypeStruct((blocks, SUB, LANES), jnp.float32)
    anywhere = pl.BlockSpec(memory_space=pltpu.HBM)
    vec = pltpu.VMEM((blocks, SUB, LANES), jnp.float32)
    dma = pltpu.SemaphoreType.DMA
    mean, comb, old_u = pl.pallas_call(
        functools.partial(kernel, n_grp, n_dev, cores, parts),
        out_shape=(vector, vector, vector),
        in_specs=[anywhere, pl.BlockSpec(memory_space=pltpu.VMEM)],
        out_specs=(anywhere, anywhere, anywhere),
        scratch_shapes=[
            pltpu.VMEM((blocks, rows, GROUP), jnp.float32),
            vec, vec, vec, vec,
            pltpu.VMEM((ROUNDS, parts, plane - 1, per // parts, SUB, LANES), jnp.float32),
            pltpu.VMEM((ROUNDS, parts, line, per // parts, SUB, LANES), jnp.float32),
            pltpu.VMEM((ROUNDS, blocks, SUB, LANES), jnp.float32),
            dma((blocks,)),
            dma((ROUNDS, parts, plane - 1)), dma((ROUNDS, parts, plane - 1)),
            dma((ROUNDS, parts, line - 1)), dma((ROUNDS, parts, line - 1)),
            dma((ROUNDS, parts, plane - 1)), dma((ROUNDS, parts, plane - 1)),
            dma((plane + 2,)),
        ],
        compiler_params=pltpu.CompilerParams(collective_id=0, has_side_effects=True),
    )(examples, labels.reshape(1, rows))
    z = shrink(mean)
    return z.reshape(width), (comb - old_u).reshape(1, width), (comb - z).reshape(1, width)


def solution(mesh):
    placed = (P(("grp", "dev"), None), P(("grp", "dev")))
    return jax.shard_map(
        functools.partial(per_device, mesh.shape["grp"], mesh.shape["dev"]),
        mesh=mesh,
        in_specs=placed,
        out_specs=(P(), P(("grp", "dev"), None), P(("grp", "dev"), None)),
        check_vma=False,
    )
```
